256 devices in a mesh: row: 8 (over x, y_lo), col: 16 (over z, core), pair: 2 (over y_hi).
Axes of the slice: x: 4, y: 4 (y_hi: 2, y_lo: 2; y = y_hi * 2 + y_lo), z: 8, core: 2. Of those that a mesh axis runs over, the one named last changes fastest.
Arguments:
- integrals: bfloat16 [8192, 32768], P('row', 'col'), may hold values from -0.03125 to 0.03125
- kept_tiles: int32 [512, 2048], P('row', 'col'), may hold values 0 or 1
- amplitudes: bfloat16 [32768, 1536], P(('col', 'row'), 'pair'), may hold values from -6 to 6
- driver: bfloat16 [8192, 1536], P(('row', 'col', 'pair')), may hold values from -6 to 6
- vir_energy: float32 [8192], P(('row', 'col', 'pair')), may hold values from 1 to 3
- occ_energy: float32 [1536], replicated, may hold values from -1.5 to -0.25
- occ_coupling: bfloat16 [1536, 1536], replicated, may hold values from -0.15625 to 0.15625
Outputs:
- increment: float32 [8192, 1536], P(('row', 'col', 'pair'))
The draws below stay inside these ranges and needn't reach their ends.
All inputs are finite; a program needn't handle non-finite values. No bound on the sum of `kept_tiles` on one device may be relied on, other than what follows from the above.
Results may differ from the reference program's by a relative error of at most 0.0011.
Values may be sent and summed in bfloat16 or wider, within the bound.
A program may use at most 64 MiB of HBM per device.

```python
import jax
import jax.numpy as jnp
from jax import lax

TILE = 16
IJ_TOTAL = 1536
PAIRS = 8192
KETS = 32768


def set_ends(result, key, least, top_value):
    extent = result.shape
    place = [jax.random.randint(jax.random.fold_in(key, axis), (), 0, extent[axis]) for axis in range(len(extent))]
    result = result.at[tuple(place)].set(least)
    longest = extent.index(max(extent))
    place[longest] = (place[longest] + 1) % extent[longest]
    return result.at[tuple(place)].set(top_value)


def levels(key, shape, split, smallest, top_value):
    gain = 1.0
    for dim, shards_of in split:
        draws = jax.random.uniform(jax.random.fold_in(jax.random.fold_in(key, 6), dim), (shards_of,), jnp.float32, smallest / len(split), top_value / len(split))
        gain = gain * jnp.repeat(jnp.exp(draws), shape[dim] // shards_of).reshape((-1,) + (1,) * (len(shape) - 1 - dim))
    return gain


def centred(rng, dims, spread, reach, pieces=(), held_as=jnp.bfloat16):
    array = spread * jax.random.normal(rng, dims, jnp.float32)
    if pieces:
        array = array * levels(rng, dims, pieces, -0.22, 0.18)
    return jnp.clip(array, -reach, reach).astype(held_as)


def setup_inputs(seed: int = 0) -> dict:
    splits = jax.random.split(jax.random.key(seed), 8)
    return {
        "integrals": centred(splits[0], (PAIRS, KETS), KETS ** -0.5, 0.03125, ((0, 8), (1, 16))),
        "kept_tiles": set_ends((jax.random.randint(splits[1], (PAIRS // TILE, KETS // TILE), 0, 4) < 3).astype(jnp.int32), jax.random.fold_in(splits[1], 1), 0, 1),
        "amplitudes": centred(splits[2], (KETS, IJ_TOTAL), 1.0, 6.0, ((0, 128), (1, 2))),
        "driver": centred(splits[3], (PAIRS, IJ_TOTAL), 1.0, 6.0, ((0, 256),)),
        "vir_energy": jnp.clip(1.0 + 2.0 * jax.random.uniform(splits[4], (PAIRS,), jnp.float32) ** levels(splits[4], (PAIRS,), ((0, 256),), -0.2, 0.2), 1.0, 3.0),
        "occ_energy": jnp.clip(jax.random.uniform(splits[5], (IJ_TOTAL,), jnp.float32, -1.5, -0.25), -1.5, -0.25),
        "occ_coupling": centred(splits[6], (IJ_TOTAL, IJ_TOTAL), IJ_TOTAL ** -0.5, 0.15625),
    }


def reference(integrals, kept_tiles, amplitudes, driver, vir_energy, occ_energy, occ_coupling):
    ampl_full = amplitudes.astype(jnp.float32)
    tile_rows = PAIRS // TILE

    def one_block(index):
        block = lax.dynamic_slice_in_dim(integrals, index * TILE, TILE, 0).astype(jnp.float32)
        keep_row = lax.dynamic_slice_in_dim(kept_tiles, index, 1, 0)[0]
        col_mask = jnp.repeat(keep_row, TILE).astype(jnp.float32)
        return jnp.dot(block * col_mask[None, :], ampl_full, precision=lax.Precision.HIGHEST)

    ladder = lax.map(one_block, jnp.arange(tile_rows, dtype=jnp.int32)).reshape(PAIRS, IJ_TOTAL)
    residual = driver.astype(jnp.float32) + ladder
    denom = vir_energy[:, None] - occ_energy[None, :]
    scaled = (residual / denom).astype(jnp.bfloat16)
    coupled = jnp.dot(scaled, occ_coupling, preferred_element_type=jnp.float32)
    return -(residual - coupled) / denom
```

```python
import jax
import jax.numpy as jnp
from jax import lax
from jax.experimental import pallas as pl
from jax.experimental.pallas import tpu as pltpu
from jax.sharding import PartitionSpec as P

MESH = pl.DeviceIdType.MESH
WIDTH = 128
FIRST = 112
HALF = 128
QUARTER = 64
AHEAD = 2
LEVELS = 32000.0


def kernel(
    integrals, kept, amplitudes, driver, vir, occ, coupling, out,
    screened, kept_v, driver_v, vir_v, occ_v, coup_v, mask, amps, part, sib, quant, scale, zin, zscale,
    total, pair_in, resid, coupled,
    load_sem, amp_sem, a_send, a_recv, d_send, d_recv, z_send, z_recv, s_send, s_recv, p_send, p_recv,
):
    chunks, rows, kets, width = amps.shape
    depth = screened.shape[1]
    sites = part.shape[1]
    row, col, pair = lax.axis_index("row"), lax.axis_index("col"), lax.axis_index("pair")
    x, y = row // 2, row % 2
    z, core = col // 2, col % 2
    ring = rows // 2

    def at(x_, y_):
        return lax.rem(x_ + ring, ring) * 2 + y_

    up, down, over = at(x + 1, y), at(x - 1, y), at(x, 1 - y)
    two = at(x + 2, y)
    up_o, down_o, two_o = at(x + 1, 1 - y), at(x - 1, 1 - y), at(x + 2, 1 - y)

    def peer(row_=None, col_=None, pair_=None):
        return (
            row if row_ is None else row_,
            col if col_ is None else col_,
            pair if pair_ is None else pair_,
        )

    to_up, to_down, to_over = peer(up), peer(down), peer(over)
    to_sib = peer(None, z * 2 + 1 - core)
    to_pair = peer(None, None, 1 - pair)

    def to_site(d):
        return peer(None, lax.rem(z + d, sites) * 2 + core)

    own_loads = []
    for j in range(chunks):
        c = pltpu.make_async_copy(
            amplitudes.at[:, pl.ds(j * width, width)], amps.at[j, row], amp_sem.at[j]
        )
        c.start()
        own_loads.append(c)
    pairs_ = (
        (kept, kept_v), (integrals, screened), (vir, vir_v), (occ, occ_v), (driver, driver_v), (coupling, coup_v),
    )
    loads = [pltpu.make_async_copy(a, b, load_sem.at[i]) for i, (a, b) in enumerate(pairs_)]
    for c in loads:
        c.start()

    barrier = pltpu.get_barrier_semaphore()
    friends = [to_up, to_down, to_over, to_sib, to_pair] + [to_site(d) for d in range(1, sites)]
    for f in friends:
        pl.semaphore_signal(barrier, inc=1, device_id=f, device_id_type=MESH)

    def hop(j, i, block, lo, hi, device):
        ref = amps.at[j, block, pl.ds(lo, hi - lo)]
        return pltpu.make_async_remote_copy(
            src_ref=ref, dst_ref=ref, send_sem=a_send.at[j, i], recv_sem=a_recv.at[j, i],
            device_id=device, device_id_type=MESH,
        )

    hops = (
        (row, down, 0, kets, to_up),
        (row, up, 0, kets, to_down),
        (row, over, 0, kets, to_over),
        (down, two, 0, HALF, to_up),
        (down, down_o, 0, FIRST, to_over),
        (up, two, HALF, kets, to_down),
        (up, up_o, 0, FIRST, to_over),
        (over, down_o, FIRST, kets, to_up),
        (over, up_o, FIRST, kets, to_down),
        (two, two_o, 0, FIRST, to_over),
        (down_o, two_o, FIRST, FIRST + QUARTER, to_up),
        (up_o, two_o, FIRST + QUARTER, kets, to_down),
    )

    def send(j, i):
        block, _, lo, hi, device = hops[i]
        hop(j, i, block, lo, hi, device).start()

    def arrived(j, i):
        _, block, lo, hi, device = hops[i]
        hop(j, i, block, lo, hi, device).wait_recv()

    def sent(j):
        for i, (block, _, lo, hi, device) in enumerate(hops):
            hop(j, i, block, lo, hi, device).wait_send()

    def first(j):
        own_loads[j].wait()
        for i in (0, 1, 2):
            send(j, i)

    def second(j):
        arrived(j, 0)
        send(j, 3)
        send(j, 4)
        arrived(j, 1)
        send(j, 5)
        send(j, 6)
        arrived(j, 2)
        send(j, 7)
        send(j, 8)

    def third(j):
        arrived(j, 7)
        send(j, 10)
        arrived(j, 8)
        send(j, 11)
        arrived(j, 3)
        send(j, 9)

    def gathered(j):
        for i in (4, 5, 6, 9, 10, 11):
            arrived(j, i)

    def sib_copy(j):
        return pltpu.make_async_remote_copy(
            src_ref=part.at[j, :, 1 - core], dst_ref=sib.at[j], send_sem=d_send.at[j], recv_sem=d_recv.at[j],
            device_id=to_sib, device_id_type=MESH,
        )

    def multiply(j):
        def step(m, carry):
            left = screened[pl.ds(m * 256, 256), :]
            right = amps[j].reshape(rows * kets, width)
            product = jnp.dot(left, right, preferred_element_type=jnp.float32)
            part[j, pl.ds(m * 2, 2)] = product.reshape(2, 2, 64, width)
            return carry

        lax.fori_loop(0, screened.shape[0] // 256, step, 0)
        sib_copy(j).start()

    def site_copy(j, d):
        return pltpu.make_async_remote_copy(
            src_ref=quant.at[j, d - 1], dst_ref=zin.at[j, d - 1],
            send_sem=z_send.at[j, d - 1], recv_sem=z_recv.at[j, d - 1],
            device_id=to_site(d), device_id_type=MESH,
        )

    def scale_copy(j, d):
        return pltpu.make_async_remote_copy(
            src_ref=scale.at[j, d - 1], dst_ref=zscale.at[j, d - 1],
            send_sem=s_send.at[j, d - 1], recv_sem=s_recv.at[j, d - 1],
            device_id=to_site(d), device_id_type=MESH,
        )

    order = sorted(range(1, sites), key=lambda d: -min(d, sites - d))

    def scatter(j):
        sib_copy(j).wait_recv()
        for d in order:
            dest = lax.rem(z + d, sites)
            value = part[j, dest, core] + sib[j, dest]
            top = jnp.maximum(jnp.max(jnp.abs(value), axis=0, keepdims=True), 1e-30)
            scale[j, d - 1] = top * (1.0 / LEVELS)
            quant[j, d - 1] = jnp.round(value * (LEVELS / top)).astype(jnp.int32).astype(jnp.int16)
            scale_copy(j, d).start()
            site_copy(j, d).start()

    def pair_copy(j):
        return pltpu.make_async_remote_copy(
            src_ref=total.at[j, pl.ds((1 - pair) * 32, 32)], dst_ref=pair_in.at[j],
            send_sem=p_send.at[j], recv_sem=p_recv.at[j],
            device_id=to_pair, device_id_type=MESH,
        )

    def collect(j):
        value = part[j, z, core] + sib[j, z]
        for d in reversed(order):
            scale_copy(j, d).wait_recv()
            site_copy(j, d).wait_recv()
            value += zin[j, d - 1].astype(jnp.int32).astype(jnp.float32) * zscale[j, d - 1]
        total[j] = value
        pair_copy(j).start()

    half = chunks * width

    def couple(j, which, ladder):
        columns = pl.ds(pl.multiple_of(which * half + j * width, width), width)
        residual = driver_v[:, columns].astype(jnp.float32) + ladder
        resid[:, columns] = residual
        scaled = (residual / (vir_col() - occ_v[:, columns])).astype(jnp.bfloat16)
        coupled[...] += jnp.dot(scaled, coup_v[columns, :], preferred_element_type=jnp.float32)

    def vir_col():
        n = vir_v.shape[1]
        eye = lax.broadcasted_iota(jnp.int32, (n, n), 0) == lax.broadcasted_iota(jnp.int32, (n, n), 1)
        return jnp.sum(jnp.where(eye, jnp.broadcast_to(vir_v[...], (n, n)), 0.0), axis=1, keepdims=True)

    def finish(j):
        couple(j, pair, total[j, pl.ds(pair * 32, 32)])
        pair_copy(j).wait_recv()
        couple(j, 1 - pair, pair_in[j])

    pl.semaphore_wait(barrier, len(friends))
    for j in range(min(AHEAD, chunks)):
        first(j)

    coupled[...] = jnp.zeros_like(coupled)
    loads[0].wait()
    tiles = kept_v.shape[1]
    tile = depth // tiles
    keep = kept_v[...].astype(jnp.float32).astype(jnp.bfloat16)
    for b in range(depth // 256):
        ket = lax.broadcasted_iota(jnp.int32, (tiles, 256), 1) + b * 256
        of = lax.broadcasted_iota(jnp.int32, (tiles, 256), 0) * tile
        spread = jnp.where((ket >= of) & (ket < of + tile), 1.0, 0.0).astype(jnp.bfloat16)
        mask[:, pl.ds(b * 256, 256)] = jnp.dot(keep, spread, preferred_element_type=jnp.float32)
    loads[1].wait()

    def screen(i, carry):
        strip = pl.ds(i * tile, tile)
        keep_row = jnp.broadcast_to(mask[pl.ds(i, 1), :], (tile, depth)).astype(jnp.bfloat16)
        screened[strip, :] = screened[strip, :] * keep_row
        return carry

    lax.fori_loop(0, kept_v.shape[0], screen, 0)

    for s in range(chunks + 2):
        if s < chunks:
            second(s)
        if 0 <= s - 1 < chunks:
            third(s - 1)
        if s + AHEAD < chunks:
            first(s + AHEAD)
        if s == 2:
            for c in loads[2:]:
                c.wait()
        if s >= 5:
            finish(s - 5)
        if s >= 4:
            collect(s - 4)
        if s >= 3:
            scatter(s - 3)
        if s >= 2:
            gathered(s - 2)
            multiply(s - 2)
            sent(s - 2)
    last = chunks - 1
    scatter(last)
    if chunks > 2:
        finish(last - 2)
    if chunks > 1:
        collect(last - 1)
        finish(last - 1)
    for j in range(chunks):
        sib_copy(j).wait_send()
        if j < last:
            pair_copy(j).wait_send()
        for d in order:
            site_copy(j, d).wait_send()
            scale_copy(j, d).wait_send()
    collect(last)
    finish(last)
    out[...] = resid[...] - coupled[...]
    pair_copy(last).wait_send()


def per_device(integrals, kept_tiles, amplitudes, driver, vir_energy, occ_energy, occ_coupling):
    bra, depth = integrals.shape
    kets, half = amplitudes.shape
    rows = depth // kets
    chunks = half // WIDTH
    sites = bra // 128
    own, whole = driver.shape
    any_ = pl.BlockSpec(memory_space=pl.ANY)
    dma = pltpu.SemaphoreType.DMA
    numerator = pl.pallas_call(
        kernel,
        out_shape=jax.ShapeDtypeStruct((own, whole), jnp.float32),
        in_specs=[any_] * 7,
        out_specs=pl.BlockSpec(memory_space=pltpu.VMEM),
        scratch_shapes=[
            pltpu.VMEM((bra, depth), jnp.bfloat16),
            pltpu.VMEM(kept_tiles.shape, jnp.int32),
            pltpu.VMEM((own, whole), jnp.bfloat16),
            pltpu.VMEM((1, own), jnp.float32),
            pltpu.VMEM((1, whole), jnp.float32),
            pltpu.VMEM((whole, whole), jnp.bfloat16),
            pltpu.VMEM((kept_tiles.shape[0], depth), jnp.float32),
            pltpu.VMEM((chunks, rows, kets, WIDTH), jnp.bfloat16),
            pltpu.VMEM((chunks, sites, 2, 64, WIDTH), jnp.float32),
            pltpu.VMEM((chunks, sites, 64, WIDTH), jnp.float32),
            pltpu.VMEM((chunks, sites - 1, 64, WIDTH), jnp.int16),
            pltpu.VMEM((chunks, sites - 1, 1, WIDTH), jnp.float32),
            pltpu.VMEM((chunks, sites - 1, 64, WIDTH), jnp.int16),
            pltpu.VMEM((chunks, sites - 1, 1, WIDTH), jnp.float32),
            pltpu.VMEM((chunks, 64, WIDTH), jnp.float32),
            pltpu.VMEM((chunks, 32, WIDTH), jnp.float32),
            pltpu.VMEM((own, whole), jnp.float32),
            pltpu.VMEM((own, whole), jnp.float32),
            dma((6,)),
            dma((chunks,)),
            dma((chunks, 12)),
            dma((chunks, 12)),
            dma((chunks,)),
            dma((chunks,)),
            dma((chunks, sites - 1)),
            dma((chunks, sites - 1)),
            dma((chunks, sites - 1)),
            dma((chunks, sites - 1)),
            dma((chunks,)),
            dma((chunks,)),
        ],
        compiler_params=pltpu.CompilerParams(
            collective_id=0, has_side_effects=True, vmem_limit_bytes=48 * 1024 * 1024
        ),
        name="ladder",
    )(
        integrals, kept_tiles, amplitudes, driver,
        vir_energy.reshape(1, own), occ_energy.reshape(1, whole), occ_coupling,
    )
    return -numerator / (vir_energy[:, None] - occ_energy[None, :])


def solution(mesh):
    place = ("row", "col", "pair")
    placed = (
        P("row", "col"),
        P("row", "col"),
        P(("col", "row"), "pair"),
        P(place, None),
        P(place),
        P(),
        P(),
    )
    return jax.shard_map(
        per_device, mesh=mesh, in_specs=placed, out_specs=P(place, None), check_vma=False
    )
```

```python
import jax
import jax.numpy as jnp
from jax import lax
from jax.experimental import pallas as pl
from jax.experimental.pallas import tpu as pltpu
from jax.sharding import PartitionSpec as P

MESH = pl.DeviceIdType.MESH
WIDTH = 128
FIRST = 112
HALF = 128
QUARTER = 64
ORDER = "SFECXTG"
LAG_T = 1
LAG_G = 2
AHEAD = 2
LEVELS = 32000.0
GROUP = (0, 0, 0, 1, 2, 3, 2, 1, 1, 2, 3, 2)


def kernel(
    integrals, kept, amplitudes, driver, vir, occ, coupling, out,
    screened, kept_v, driver_v, vir_v, occ_v, coup_v, mask, amps, part, sib, quant, scale, zin, zscale,
    total, pair_in, resid, coupled,
    load_sem, sends, a_recv, d_recv, z_recv, s_recv, p_recv, ready,
):
    chunks, rows, kets, width = amps.shape
    depth = screened.shape[1]
    sites = part.shape[1]
    row, col, pair = lax.axis_index("row"), lax.axis_index("col"), lax.axis_index("pair")
    x, y = row // 2, row % 2
    z, core = col // 2, col % 2
    ring = rows // 2

    def at(x_, y_):
        return lax.rem(x_ + ring, ring) * 2 + y_

    up, down, over = at(x + 1, y), at(x - 1, y), at(x, 1 - y)
    two = at(x + 2, y)
    up_o, down_o, two_o = at(x + 1, 1 - y), at(x - 1, 1 - y), at(x + 2, 1 - y)

    def peer(row_=None, col_=None, pair_=None):
        return (
            row if row_ is None else row_,
            col if col_ is None else col_,
            pair if pair_ is None else pair_,
        )

    to_up, to_down, to_over = peer(up), peer(down), peer(over)
    to_sib = peer(None, z * 2 + 1 - core)
    to_pair = peer(None, None, 1 - pair)

    def to_site(d):
        return peer(None, lax.rem(z + d, sites) * 2 + core)

    for j in range(chunks):
        pltpu.make_async_copy(
            amplitudes.at[:, pl.ds(j * width, width)], amps.at[j, row], load_sem.at[6]
        ).start()
    pairs_ = (
        (kept, kept_v), (integrals, screened), (vir, vir_v), (occ, occ_v), (driver, driver_v), (coupling, coup_v),
    )
    loads = [pltpu.make_async_copy(a, b, load_sem.at[i]) for i, (a, b) in enumerate(pairs_)]
    for c in loads:
        c.start()

    barrier = pltpu.get_barrier_semaphore()
    friends = [to_up, to_down, to_over, to_sib, to_pair, to_site(1), to_site(sites - 1)]
    for f in friends:
        pl.semaphore_signal(barrier, inc=1, device_id=f, device_id_type=MESH)

    def tell(n):
        for d in (1, sites - 1):
            pl.semaphore_signal(ready.at[n], inc=1, device_id=to_site(d), device_id_type=MESH)

    def told(n):
        pl.semaphore_wait(ready.at[n], 2)

    def hop(j, i, block, lo, hi, device):
        ref = amps.at[j, block, pl.ds(lo, hi - lo)]
        return pltpu.make_async_remote_copy(
            src_ref=ref, dst_ref=ref, send_sem=sends.at[0], recv_sem=a_recv.at[j, GROUP[i]],
            device_id=device, device_id_type=MESH,
        )

    hops = (
        (row, down, 0, kets, to_up),
        (row, up, 0, kets, to_down),
        (row, over, 0, kets, to_over),
        (down, two, 0, HALF, to_up),
        (down, down_o, 0, FIRST, to_over),
        (up, two, HALF, kets, to_down),
        (up, up_o, 0, FIRST, to_over),
        (over, down_o, FIRST, kets, to_up),
        (over, up_o, FIRST, kets, to_down),
        (two, two_o, 0, FIRST, to_over),
        (down_o, two_o, FIRST, FIRST + QUARTER, to_up),
        (up_o, two_o, FIRST + QUARTER, kets, to_down),
    )

    def send(j, i):
        block, _, lo, hi, device = hops[i]
        hop(j, i, block, lo, hi, device).start()

    def landed(ref, sem):
        pltpu.make_async_copy(ref, ref, sem).wait()

    def arrived(j, group):
        count = sum(hi - lo for (_, _, lo, hi, _), g in zip(hops, GROUP) if g == group)
        parts_ = next(n for n in range(1, rows) if count % (n * 16) == 0 and count // n <= kets)
        landed(amps.at[j, pl.ds(0, parts_), pl.ds(0, count // parts_)], a_recv.at[j, group])

    def first(j):
        for i in (0, 1, 2):
            send(j, i)

    def second(j):
        arrived(j, 0)
        for i in (3, 7, 8, 5, 4, 6):
            send(j, i)

    def third(j):
        arrived(j, 1)
        for i in (10, 11, 9):
            send(j, i)

    def gathered(j):
        arrived(j, 2)
        arrived(j, 3)

    def site(d):
        return lax.rem(z + d, sites)

    last = chunks - 1

    def sib_sem(j, d):
        return j if j < last else last + min(d, sites - 1 - d)

    def sib_copy(j, d):
        return pltpu.make_async_remote_copy(
            src_ref=part.at[j, site(d), 1 - core], dst_ref=sib.at[j, site(d)],
            send_sem=sends.at[1], recv_sem=d_recv.at[sib_sem(j, d)],
            device_id=to_sib, device_id_type=MESH,
        )

    def multiply(j):
        for d in range(sites // 2, sites):
            both = (d, sites - 1 - d)
            left = jnp.concatenate([screened[pl.ds(site(e) * 128, 128), :] for e in both], axis=0)
            right = amps[j].reshape(rows * kets, width)
            product = jnp.dot(left, right, preferred_element_type=jnp.float32).reshape(2, 2, 64, width)
            for i, e in enumerate(both):
                part[j, site(e)] = product[i]
                sib_copy(j, e).start()

    def site_copy(j, d):
        return pltpu.make_async_remote_copy(
            src_ref=quant.at[j, d - 1], dst_ref=zin.at[j, d - 1],
            send_sem=sends.at[2], recv_sem=z_recv.at[j],
            device_id=to_site(d), device_id_type=MESH,
        )

    def scale_copy(j, d):
        return pltpu.make_async_remote_copy(
            src_ref=scale.at[j, d - 1], dst_ref=zscale.at[j, d - 1],
            send_sem=sends.at[3], recv_sem=s_recv.at[j],
            device_id=to_site(d), device_id_type=MESH,
        )

    order = [e for d in range(sites // 2, sites) for e in (d, sites - 1 - d) if e]

    def scatter(j):
        if j < last:
            with jax.named_scope("sibwait"):
                landed(sib.at[j], d_recv.at[j])
        for d in order:
            if j == last and d >= sites // 2:
                with jax.named_scope("sibwait"):
                    landed(sib.at[j, pl.ds(0, 2)], d_recv.at[sib_sem(j, d)])
            value = part[j, site(d), core] + sib[j, site(d)]
            top = jnp.maximum(jnp.max(jnp.abs(value), axis=0, keepdims=True), 1e-30)
            scale[j, d - 1] = top * (1.0 / LEVELS)
            quant[j, d - 1] = jnp.round(value * (LEVELS / top)).astype(jnp.int32).astype(jnp.int16)
            scale_copy(j, d).start()
            site_copy(j, d).start()

    def pair_copy(j):
        return pltpu.make_async_remote_copy(
            src_ref=total.at[j, pl.ds((1 - pair) * 32, 32)], dst_ref=pair_in.at[j],
            send_sem=sends.at[4], recv_sem=p_recv.at[j],
            device_id=to_pair, device_id_type=MESH,
        )

    def collect(j):
        value = part[j, z, core] + sib[j, z]
        with jax.named_scope("sitewait"):
            landed(zscale.at[j], s_recv.at[j])
            landed(zin.at[j], z_recv.at[j])
        for d in reversed(order):
            value += zin[j, d - 1].astype(jnp.int32).astype(jnp.float32) * zscale[j, d - 1]
        total[j] = value
        pair_copy(j).start()

    half = chunks * width

    def couple(j, which, ladder):
        columns = pl.ds(pl.multiple_of(which * half + j * width, width), width)
        residual = driver_v[:, columns].astype(jnp.float32) + ladder
        resid[:, columns] = residual
        scaled = (residual / (vir_col() - occ_v[columns].reshape(1, width))).astype(jnp.bfloat16)
        coupled[...] += jnp.dot(scaled, coup_v[columns, :], preferred_element_type=jnp.float32)

    def vir_col():
        n = vir_v.shape[0]
        eye = lax.broadcasted_iota(jnp.int32, (n, n), 0) == lax.broadcasted_iota(jnp.int32, (n, n), 1)
        return jnp.sum(jnp.where(eye, jnp.broadcast_to(vir_v[...].reshape(1, n), (n, n)), 0.0), axis=1, keepdims=True)

    def finish(j):
        couple(j, pair, total[j, pl.ds(pair * 32, 32)])
        with jax.named_scope("pairwait"):
            pair_copy(j).wait_recv()
        couple(j, 1 - pair, pair_in[j])

    with jax.named_scope("barrier"):
        pl.semaphore_wait(barrier, len(friends))
    landed(amps.at[:, row], load_sem.at[6])
    with jax.named_scope("first"):
        for j in range(min(AHEAD, chunks)):
            first(j)
    tell(0)

    coupled[...] = jnp.zeros_like(coupled)
    loads[0].wait()
    tiles = kept_v.shape[1]
    tile = depth // tiles
    keep = kept_v[...].astype(jnp.float32).astype(jnp.bfloat16)
    for b in range(depth // 256):
        ket = lax.broadcasted_iota(jnp.int32, (tiles, 256), 1) + b * 256
        of = lax.broadcasted_iota(jnp.int32, (tiles, 256), 0) * tile
        spread = jnp.where((ket >= of) & (ket < of + tile), 1.0, 0.0).astype(jnp.bfloat16)
        mask[:, pl.ds(b * 256, 256)] = jnp.dot(keep, spread, preferred_element_type=jnp.float32)
    loads[1].wait()

    def screen(i, carry):
        strip = pl.ds(i * tile, tile)
        keep_row = jnp.broadcast_to(mask[pl.ds(i, 1), :], (tile, depth)).astype(jnp.bfloat16)
        screened[strip, :] = screened[strip, :] * keep_row
        return carry

    with jax.named_scope("screen"):
        lax.fori_loop(0, kept_v.shape[0], screen, 0)
    def product(j):
        with jax.named_scope("gathered"):
            gathered(j)
        with jax.named_scope("dot"):
            multiply(j)

    def named(name, f):
        def call(j):
            with jax.named_scope(name):
                f(j)

        return call

    steps = {
        "S": (0, named("second", second)),
        "F": (-AHEAD, first),
        "T": (LAG_T, named("third", third)),
        "G": (LAG_G, product),
        "X": (LAG_G + 1, scatter),
        "C": (LAG_G + 3, collect),
        "E": (LAG_G + 5, finish),
    }
    done = dict.fromkeys(steps, -1)
    done["F"] = AHEAD - 1
    for s in range(chunks + LAG_G):
        for name in ORDER:
            lag, step = steps[name]
            j = s - lag
            if 0 <= j < chunks and j > done[name]:
                step(j)
                done[name] = j
        if s < sites // 2 - 1:
            told(s)
            if s + 1 < sites // 2 - 1:
                tell(s + 1)
        if s == 2:
            for c in loads[2:]:
                c.wait()
    for j in range(done["X"] + 1, chunks):
        scatter(j)
    for j in range(done["C"] + 1, chunks):
        if j == last:
            landed(amps.at[:, pl.ds(0, rows - 1)], sends.at[0])
            landed(sib, sends.at[1])
        collect(j)
        while done["E"] < j - 1:
            done["E"] += 1
            finish(done["E"])
    landed(quant, sends.at[2])
    landed(scale, sends.at[3])
    with jax.named_scope("finlast"):
        finish(last)
    with jax.named_scope("out"):
        resid[...] = resid[...] - coupled[...]
        oc = pltpu.make_async_copy(resid, out, load_sem.at[6])
        oc.start()
        oc.wait()
    with jax.named_scope("pairsent"):
        landed(pair_in, sends.at[4])


def per_device(integrals, kept_tiles, amplitudes, driver, vir_energy, occ_energy, occ_coupling):
    bra, depth = integrals.shape
    kets, half = amplitudes.shape
    rows = depth // kets
    chunks = half // WIDTH
    sites = bra // 128
    own, whole = driver.shape
    any_ = pl.BlockSpec(memory_space=pltpu.HBM)
    dma = pltpu.SemaphoreType.DMA
    numerator = pl.pallas_call(
        kernel,
        out_shape=jax.ShapeDtypeStruct((own, whole), jnp.float32),
        in_specs=[any_] * 7,
        out_specs=any_,
        scratch_shapes=[
            pltpu.VMEM((bra, depth), jnp.bfloat16),
            pltpu.VMEM(kept_tiles.shape, jnp.int32),
            pltpu.VMEM((own, whole), jnp.bfloat16),
            pltpu.VMEM((own,), jnp.float32),
            pltpu.VMEM((whole,), jnp.float32),
            pltpu.VMEM((whole, whole), jnp.bfloat16),
            pltpu.VMEM((kept_tiles.shape[0], depth), jnp.float32),
            pltpu.VMEM((chunks, rows, kets, WIDTH), jnp.bfloat16),
            pltpu.VMEM((chunks, sites, 2, 64, WIDTH), jnp.float32),
            pltpu.VMEM((chunks, sites, 64, WIDTH), jnp.float32),
            pltpu.VMEM((chunks, sites - 1, 64, WIDTH), jnp.int16),
            pltpu.VMEM((chunks, sites - 1, 1, WIDTH), jnp.float32),
            pltpu.VMEM((chunks, sites - 1, 64, WIDTH), jnp.int16),
            pltpu.VMEM((chunks, sites - 1, 1, WIDTH), jnp.float32),
            pltpu.VMEM((chunks, 64, WIDTH), jnp.float32),
            pltpu.VMEM((chunks, 32, WIDTH), jnp.float32),
            pltpu.VMEM((own, whole), jnp.float32),
            pltpu.VMEM((own, whole), jnp.float32),
            dma((7,)),
            dma((5,)),
            dma((chunks, 4)),
            dma((chunks + sites // 2,)),
            dma((chunks,)),
            dma((chunks,)),
            dma((chunks,)),
            pltpu.SemaphoreType.REGULAR((sites // 2 - 1,)),
        ],
        compiler_params=pltpu.CompilerParams(
            collective_id=0, has_side_effects=True, vmem_limit_bytes=60 * 1024 * 1024
        ),
        name="ladder",
    )(
        integrals, kept_tiles, amplitudes, driver,
        vir_energy, occ_energy, occ_coupling,
    )
    return -numerator / (vir_energy[:, None] - occ_energy[None, :])


def solution(mesh):
    place = ("row", "col", "pair")
    placed = (
        P("row", "col"),
        P("row", "col"),
        P(("col", "row"), "pair"),
        P(place, None),
        P(place),
        P(),
        P(),
    )
    return jax.shard_map(
        per_device, mesh=mesh, in_specs=placed, out_specs=P(place, None), check_vma=False
    )
```

```python
import jax
import jax.numpy as jnp
from jax import lax
from jax.experimental import pallas as pl
from jax.experimental.pallas import tpu as pltpu
from jax.sharding import PartitionSpec as P

MESH = pl.DeviceIdType.MESH
WIDTH = 128
FIRST = 112
HALF = 128
QUARTER = 64
ORDER = "SFECXTGR"
LAG_T = 1
FAR = 4
LAG_G = 2
AHEAD = 2
LEVELS = 32000.0
GROUP = (0, 0, 0, 1, 2, 3, 2, 1, 1, 2, 3, 2)


def kernel(
    integrals, kept, amplitudes, driver, vir, occ, coupling, out,
    screened, kept_v, driver_v, vir_v, occ_v, coup_v, mask, amps, part, sib, quant, scale, zin, zscale,
    total, pair_in, far, far_scale, resid, coupled,
    load_sem, sends, a_recv, d_recv, z_recv, s_recv, p_recv, f_recv, ready,
):
    chunks, rows, kets, width = amps.shape
    depth = screened.shape[1]
    sites = part.shape[1]
    row, col, pair = lax.axis_index("row"), lax.axis_index("col"), lax.axis_index("pair")
    x, y = row // 2, row % 2
    z, core = col // 2, col % 2
    ring = rows // 2

    def at(x_, y_):
        return lax.rem(x_ + ring, ring) * 2 + y_

    up, down, over = at(x + 1, y), at(x - 1, y), at(x, 1 - y)
    two = at(x + 2, y)
    up_o, down_o, two_o = at(x + 1, 1 - y), at(x - 1, 1 - y), at(x + 2, 1 - y)

    def peer(row_=None, col_=None, pair_=None):
        return (
            row if row_ is None else row_,
            col if col_ is None else col_,
            pair if pair_ is None else pair_,
        )

    to_up, to_down, to_over = peer(up), peer(down), peer(over)
    to_sib = peer(None, z * 2 + 1 - core)
    to_pair = peer(None, None, 1 - pair)

    def to_site(d):
        return peer(None, lax.rem(z + d, sites) * 2 + core)

    for j in range(chunks):
        pltpu.make_async_copy(
            amplitudes.at[:, pl.ds(j * width, width)], amps.at[j, row], load_sem.at[6]
        ).start()
    pairs_ = (
        (kept, kept_v), (integrals, screened), (vir, vir_v), (occ, occ_v), (driver, driver_v), (coupling, coup_v),
    )
    loads = [pltpu.make_async_copy(a, b, load_sem.at[i]) for i, (a, b) in enumerate(pairs_)]
    for c in loads:
        c.start()

    barrier = pltpu.get_barrier_semaphore()
    friends = [to_up, to_down, to_over, to_sib, to_pair, to_site(1), to_site(sites - 1)]
    for f in friends:
        pl.semaphore_signal(barrier, inc=1, device_id=f, device_id_type=MESH)

    def tell(n):
        for d in (1, sites - 1):
            pl.semaphore_signal(ready.at[n], inc=1, device_id=to_site(d), device_id_type=MESH)

    def told(n):
        pl.semaphore_wait(ready.at[n], 2)

    def hop(j, i, block, lo, hi, device):
        ref = amps.at[j, block, pl.ds(lo, hi - lo)]
        return pltpu.make_async_remote_copy(
            src_ref=ref, dst_ref=ref, send_sem=sends.at[0], recv_sem=a_recv.at[j, GROUP[i]],
            device_id=device, device_id_type=MESH,
        )

    hops = (
        (row, down, 0, kets, to_up),
        (row, up, 0, kets, to_down),
        (row, over, 0, kets, to_over),
        (down, two, 0, HALF, to_up),
        (down, down_o, 0, FIRST, to_over),
        (up, two, HALF, kets, to_down),
        (up, up_o, 0, FIRST, to_over),
        (over, down_o, FIRST, kets, to_up),
        (over, up_o, FIRST, kets, to_down),
        (two, two_o, 0, FIRST, to_over),
        (down_o, two_o, FIRST, FIRST + QUARTER, to_up),
        (up_o, two_o, FIRST + QUARTER, kets, to_down),
    )

    def send(j, i):
        block, _, lo, hi, device = hops[i]
        hop(j, i, block, lo, hi, device).start()

    def landed(ref, sem):
        pltpu.make_async_copy(ref, ref, sem).wait()

    def arrived(j, group):
        count = sum(hi - lo for (_, _, lo, hi, _), g in zip(hops, GROUP) if g == group)
        parts_ = next(n for n in range(1, rows) if count % (n * 16) == 0 and count // n <= kets)
        landed(amps.at[j, pl.ds(0, parts_), pl.ds(0, count // parts_)], a_recv.at[j, group])

    def first(j):
        for i in (0, 1, 2):
            send(j, i)

    def second(j):
        arrived(j, 0)
        for i in (3, 7, 8, 5, 4, 6):
            send(j, i)

    def third(j):
        arrived(j, 1)
        for i in (10, 11, 9):
            send(j, i)

    def gathered(j):
        arrived(j, 2)
        arrived(j, 3)

    def site(d):
        return lax.rem(z + d, sites)

    last = chunks - 1

    def sib_sem(j, d):
        return j if j < last else last + min(d, sites - 1 - d)

    def sib_copy(j, d):
        return pltpu.make_async_remote_copy(
            src_ref=part.at[j, site(d), 1 - core], dst_ref=sib.at[j, site(d)],
            send_sem=sends.at[1], recv_sem=d_recv.at[sib_sem(j, d)],
            device_id=to_sib, device_id_type=MESH,
        )

    def multiply(j):
        for d in range(sites // 2, sites):
            both = (d, sites - 1 - d)
            left = jnp.concatenate([screened[pl.ds(site(e) * 128, 128), :] for e in both], axis=0)
            right = amps[j].reshape(rows * kets, width)
            product = jnp.dot(left, right, preferred_element_type=jnp.float32).reshape(2, 2, 64, width)
            for i, e in enumerate(both):
                part[j, site(e)] = product[i]
                sib_copy(j, e).start()

    def summed(j, d):
        return part[j, site(d), core] + sib[j, site(d)]

    def encode(j, slot, value):
        top = jnp.maximum(jnp.max(jnp.abs(value), axis=0, keepdims=True), 1e-30)
        scale[j, slot] = top * (1.0 / LEVELS)
        quant[j, slot] = jnp.round(value * (LEVELS / top)).astype(jnp.int32).astype(jnp.int16)

    def decode(code, factor):
        return code.astype(jnp.int32).astype(jnp.float32) * factor

    def message(j, slot, inbox, factor, lo, hi, d, group):
        device = to_site(d)
        return (
            pltpu.make_async_remote_copy(
                src_ref=scale.at[j, slot], dst_ref=zscale.at[j, factor],
                send_sem=sends.at[3], recv_sem=s_recv.at[j, group], device_id=device, device_id_type=MESH,
            ),
            pltpu.make_async_remote_copy(
                src_ref=quant.at[j, slot, pl.ds(lo, hi - lo)], dst_ref=zin.at[j, inbox, pl.ds(lo, hi - lo)],
                send_sem=sends.at[2], recv_sem=z_recv.at[j, group], device_id=device, device_id_type=MESH,
            ),
        )

    def post(*args):
        for c in message(*args):
            c.start()

    def await_sib(j):
        with jax.named_scope("sibwait"):
            landed(sib.at[j], d_recv.at[j])

    def scatter(j):
        await_sib(j)
        encode(j, 2, summed(j, 4))
        post(j, 2, 2, 2, 0, 32, 2, 0)
        post(j, 2, 2, 3, 32, 64, 6, 0)
        encode(j, 0, summed(j, 3))
        post(j, 0, 0, 0, 0, 64, 1, 0)
        encode(j, 1, summed(j, 5))
        post(j, 1, 1, 1, 0, 64, 7, 0)
        encode(j, 3, summed(j, 1))
        post(j, 3, 3, 4, 0, 64, 1, 1)
        encode(j, 4, summed(j, 7))
        post(j, 4, 4, 5, 0, 64, 7, 1)

    def relay(j):
        with jax.named_scope("relaywait"):
            landed(zscale.at[j, pl.ds(0, 4)], s_recv.at[j, 0])
            landed(zin.at[j, pl.ds(0, 3)], z_recv.at[j, 0])
        ahead = summed(j, 2) + decode(zin[j, 0], zscale[j, 0])
        top = decode(zin[j, 2, 0:32], zscale[j, 2])
        encode(j, 5, jnp.concatenate([ahead[0:32] + top, ahead[32:64]], axis=0))
        post(j, 5, 5, 6, 0, 64, 2, 1)
        behind = summed(j, 6) + decode(zin[j, 1], zscale[j, 1])
        low = decode(zin[j, 2, 32:64], zscale[j, 3])
        encode(j, 6, jnp.concatenate([behind[0:32], behind[32:64] + low], axis=0))
        post(j, 6, 6, 7, 0, 64, 6, 1)

    def pair_copy(j):
        return pltpu.make_async_remote_copy(
            src_ref=total.at[j, pl.ds((1 - pair) * 32, 32)], dst_ref=pair_in.at[j],
            send_sem=sends.at[4], recv_sem=p_recv.at[j],
            device_id=to_pair, device_id_type=MESH,
        )

    def collect(j):
        value = summed(j, 0)
        with jax.named_scope("sitewait"):
            landed(zscale.at[j, pl.ds(4, 4)], s_recv.at[j, 1])
            landed(zin.at[j, pl.ds(3, 4)], z_recv.at[j, 1])
        for i in range(4):
            value += decode(zin[j, 3 + i], zscale[j, 4 + i])
        total[j] = value
        pair_copy(j).start()

    near = chunks - FAR

    def far_copies(j, d, other):
        whom = 1 - pair if other else pair
        device = (row, site(d) * 2 + core, whom)
        f = j - near
        return (
            pltpu.make_async_remote_copy(
                src_ref=scale.at[j, d], dst_ref=far_scale.at[f, other, d],
                send_sem=sends.at[5 + other], recv_sem=f_recv.at[f, other], device_id=device, device_id_type=MESH,
            ),
            pltpu.make_async_remote_copy(
                src_ref=quant.at[j, d, pl.ds(whom * 32, 32)], dst_ref=far.at[f, other, d],
                send_sem=sends.at[7 + other], recv_sem=f_recv.at[f, 2 + other], device_id=device, device_id_type=MESH,
            ),
        )

    def scatter_far(j):
        if j < last:
            await_sib(j)
        for d in range(sites // 2, sites):
            if j == last:
                with jax.named_scope("sibwait"):
                    landed(sib.at[j, pl.ds(0, 2)], d_recv.at[sib_sem(j, d)])
            for e in (d, sites - 1 - d):
                encode(j, e, summed(j, e))
                for other in (1, 0) if e else (1,):
                    for c in far_copies(j, e, other):
                        c.start()

    def finish_far(j):
        f = j - near
        for other in (0, 1):
            first_ = 0 if other else 1
            with jax.named_scope("farwait"):
                landed(far_scale.at[f, other, pl.ds(first_, sites - first_)], f_recv.at[f, other])
                landed(far.at[f, other, pl.ds(first_, sites - first_)], f_recv.at[f, 2 + other])
            ladder = decode(far[f, other, first_], far_scale[f, other, first_])
            for d in range(first_ + 1, sites):
                ladder += decode(far[f, other, d], far_scale[f, other, d])
            if not other:
                ladder += part[j, z, core, pl.ds(pair * 32, 32)] + sib[j, z, pl.ds(pair * 32, 32)]
            couple(j, 1 - pair if other else pair, ladder)

    def far_sent():
        for other in (0, 1):
            first_ = 0 if other else 1
            landed(far_scale.at[:, other, pl.ds(first_, sites - first_)], sends.at[5 + other])
            landed(far.at[:, other, pl.ds(first_, sites - first_)], sends.at[7 + other])

    half = chunks * width

    def couple(j, which, ladder):
        columns = pl.ds(pl.multiple_of(which * half + j * width, width), width)
        residual = driver_v[:, columns].astype(jnp.float32) + ladder
        resid[:, columns] = residual
        scaled = (residual / (vir_col() - occ_v[columns].reshape(1, width))).astype(jnp.bfloat16)
        coupled[...] += jnp.dot(scaled, coup_v[columns, :], preferred_element_type=jnp.float32)

    def vir_col():
        n = vir_v.shape[0]
        eye = lax.broadcasted_iota(jnp.int32, (n, n), 0) == lax.broadcasted_iota(jnp.int32, (n, n), 1)
        return jnp.sum(jnp.where(eye, jnp.broadcast_to(vir_v[...].reshape(1, n), (n, n)), 0.0), axis=1, keepdims=True)

    def finish(j):
        couple(j, pair, total[j, pl.ds(pair * 32, 32)])
        with jax.named_scope("pairwait"):
            pair_copy(j).wait_recv()
        couple(j, 1 - pair, pair_in[j])

    with jax.named_scope("barrier"):
        pl.semaphore_wait(barrier, len(friends))
    landed(amps.at[:, row], load_sem.at[6])
    with jax.named_scope("first"):
        for j in range(min(AHEAD, chunks)):
            first(j)
    tell(0)

    coupled[...] = jnp.zeros_like(coupled)
    loads[0].wait()
    tiles = kept_v.shape[1]
    tile = depth // tiles
    keep = kept_v[...].astype(jnp.float32).astype(jnp.bfloat16)
    for b in range(depth // 256):
        ket = lax.broadcasted_iota(jnp.int32, (tiles, 256), 1) + b * 256
        of = lax.broadcasted_iota(jnp.int32, (tiles, 256), 0) * tile
        spread = jnp.where((ket >= of) & (ket < of + tile), 1.0, 0.0).astype(jnp.bfloat16)
        mask[:, pl.ds(b * 256, 256)] = jnp.dot(keep, spread, preferred_element_type=jnp.float32)
    loads[1].wait()

    def screen(i, carry):
        strip = pl.ds(i * tile, tile)
        keep_row = jnp.broadcast_to(mask[pl.ds(i, 1), :], (tile, depth)).astype(jnp.bfloat16)
        screened[strip, :] = screened[strip, :] * keep_row
        return carry

    with jax.named_scope("screen"):
        lax.fori_loop(0, kept_v.shape[0], screen, 0)
    def product(j):
        with jax.named_scope("gathered"):
            gathered(j)
        with jax.named_scope("dot"):
            multiply(j)

    def named(name, f):
        def call(j):
            with jax.named_scope(name):
                f(j)

        return call

    steps = {
        "S": (0, named("second", second)),
        "F": (-AHEAD, first),
        "T": (LAG_T, named("third", third)),
        "G": (LAG_G, product),
        "X": (LAG_G + 1, lambda j: scatter(j) if j < near else scatter_far(j)),
        "R": (LAG_G + 2, relay),
        "C": (LAG_G + 4, collect),
        "E": (LAG_G + 5, finish),
    }
    done = dict.fromkeys(steps, -1)
    done["F"] = AHEAD - 1
    for s in range(chunks + LAG_G):
        for name in ORDER:
            lag, step = steps[name]
            j = s - lag
            if 0 <= j < (near if name in "RCE" else chunks) and j > done[name]:
                step(j)
                done[name] = j
        if s < sites // 2 - 1:
            told(s)
            if s + 1 < sites // 2 - 1:
                tell(s + 1)
        if s == 2:
            pl.semaphore_signal(ready.at[sites // 2 - 1], inc=1, device_id=to_pair, device_id_type=MESH)
            for c in loads[2:]:
                c.wait()
    pl.semaphore_wait(ready.at[sites // 2 - 1], 1)
    for j in range(done["X"] + 1, chunks):
        steps["X"][1](j)
    for j in range(done["R"] + 1, near):
        relay(j)
    for j in range(done["C"] + 1, near):
        while done["E"] < j - 2:
            done["E"] += 1
            finish(done["E"])
        collect(j)
    landed(amps.at[:, pl.ds(0, rows - 1)], sends.at[0])
    landed(sib, sends.at[1])
    landed(zin, sends.at[2])
    landed(zscale, sends.at[3])
    for j in range(done["E"] + 1, near - 1):
        finish(j)
    for j in range(near, last):
        finish_far(j)
    finish(near - 1)
    far_sent()
    landed(pair_in.at[pl.ds(0, near)], sends.at[4])
    finish_far(last)
    with jax.named_scope("out"):
        resid[...] = resid[...] - coupled[...]
        oc = pltpu.make_async_copy(resid, out, load_sem.at[6])
        oc.start()
        oc.wait()


def per_device(integrals, kept_tiles, amplitudes, driver, vir_energy, occ_energy, occ_coupling):
    bra, depth = integrals.shape
    kets, half = amplitudes.shape
    rows = depth // kets
    chunks = half // WIDTH
    sites = bra // 128
    own, whole = driver.shape
    any_ = pl.BlockSpec(memory_space=pltpu.HBM)
    dma = pltpu.SemaphoreType.DMA
    numerator = pl.pallas_call(
        kernel,
        out_shape=jax.ShapeDtypeStruct((own, whole), jnp.float32),
        in_specs=[any_] * 7,
        out_specs=any_,
        scratch_shapes=[
            pltpu.VMEM((bra, depth), jnp.bfloat16),
            pltpu.VMEM(kept_tiles.shape, jnp.int32),
            pltpu.VMEM((own, whole), jnp.bfloat16),
            pltpu.VMEM((own,), jnp.float32),
            pltpu.VMEM((whole,), jnp.float32),
            pltpu.VMEM((whole, whole), jnp.bfloat16),
            pltpu.VMEM((kept_tiles.shape[0], depth), jnp.float32),
            pltpu.VMEM((chunks, rows, kets, WIDTH), jnp.bfloat16),
            pltpu.VMEM((chunks, sites, 2, 64, WIDTH), jnp.float32),
            pltpu.VMEM((chunks, sites, 64, WIDTH), jnp.float32),
            pltpu.VMEM((chunks, sites, 64, WIDTH), jnp.int16),
            pltpu.VMEM((chunks, sites, 1, WIDTH), jnp.float32),
            pltpu.VMEM((chunks - FAR, 7, 64, WIDTH), jnp.int16),
            pltpu.VMEM((chunks - FAR, 8, 1, WIDTH), jnp.float32),
            pltpu.VMEM((chunks, 64, WIDTH), jnp.float32),
            pltpu.VMEM((chunks, 32, WIDTH), jnp.float32),
            pltpu.VMEM((FAR, 2, sites, 32, WIDTH), jnp.int16),
            pltpu.VMEM((FAR, 2, sites, 1, WIDTH), jnp.float32),
            pltpu.VMEM((own, whole), jnp.float32),
            pltpu.VMEM((own, whole), jnp.float32),
            dma((7,)),
            dma((9,)),
            dma((chunks, 4)),
            dma((chunks + sites // 2,)),
            dma((chunks, 2)),
            dma((chunks, 2)),
            dma((chunks,)),
            dma((FAR, 4)),
            pltpu.SemaphoreType.REGULAR((sites // 2,)),
        ],
        compiler_params=pltpu.CompilerParams(
            collective_id=0, has_side_effects=True, vmem_limit_bytes=60 * 1024 * 1024
        ),
        name="ladder",
    )(
        integrals, kept_tiles, amplitudes, driver,
        vir_energy, occ_energy, occ_coupling,
    )
    return -numerator / (vir_energy[:, None] - occ_energy[None, :])


def solution(mesh):
    place = ("row", "col", "pair")
    placed = (
        P("row", "col"),
        P("row", "col"),
        P(("col", "row"), "pair"),
        P(place, None),
        P(place),
        P(),
        P(),
    )
    return jax.shard_map(
        per_device, mesh=mesh, in_specs=placed, out_specs=P(place, None), check_vma=False
    )
```

```python
import jax
import jax.numpy as jnp
from jax import lax
from jax.experimental import pallas as pl
from jax.experimental.pallas import tpu as pltpu
from jax.sharding import PartitionSpec as P

MESH = pl.DeviceIdType.MESH
WIDTH = 128
FIRST = 112
HALF = 128
QUARTER = 64
ORDER = "SFXTGRCE"
LAG_T = 1
FAR = 4
LAG_G = 2
AHEAD = 2
LEVELS = 32000.0
GROUP = (0, 0, 0, 1, 2, 3, 2, 1, 1, 2, 3, 2)


def kernel(
    integrals, kept, amplitudes, driver, vir, occ, coupling, out,
    screened, kept_v, driver_v, vir_v, occ_v, coup_v, mask, amps, part, sib, quant, scale, zin, zscale,
    total, pair_in, far, far_scale, resid, coupled,
    load_sem, sends, a_recv, d_recv, z_recv, s_recv, p_recv, f_recv, ready,
):
    chunks, rows, kets, width = amps.shape
    depth = screened.shape[1]
    sites = part.shape[1]
    row, col, pair = lax.axis_index("row"), lax.axis_index("col"), lax.axis_index("pair")
    x, y = row // 2, row % 2
    z, core = col // 2, col % 2
    ring = rows // 2

    def at(x_, y_):
        return lax.rem(x_ + ring, ring) * 2 + y_

    up, down, over = at(x + 1, y), at(x - 1, y), at(x, 1 - y)
    two = at(x + 2, y)
    up_o, down_o, two_o = at(x + 1, 1 - y), at(x - 1, 1 - y), at(x + 2, 1 - y)

    def peer(row_=None, col_=None, pair_=None):
        return (
            row if row_ is None else row_,
            col if col_ is None else col_,
            pair if pair_ is None else pair_,
        )

    to_up, to_down, to_over = peer(up), peer(down), peer(over)
    to_sib = peer(None, z * 2 + 1 - core)
    to_pair = peer(None, None, 1 - pair)

    def to_site(d):
        return peer(None, lax.rem(z + d, sites) * 2 + core)

    for j in range(chunks):
        pltpu.make_async_copy(
            amplitudes.at[:, pl.ds(j * width, width)], amps.at[j, row], load_sem.at[6]
        ).start()
    pairs_ = (
        (kept, kept_v), (integrals, screened), (vir, vir_v), (occ, occ_v), (driver, driver_v), (coupling, coup_v),
    )
    loads = [pltpu.make_async_copy(a, b, load_sem.at[i]) for i, (a, b) in enumerate(pairs_)]
    for c in loads:
        c.start()

    barrier = pltpu.get_barrier_semaphore()
    friends = [to_up, to_down, to_over, to_sib, to_pair, to_site(1), to_site(sites - 1)]
    for f in friends:
        pl.semaphore_signal(barrier, inc=1, device_id=f, device_id_type=MESH)

    def tell(n):
        for d in (1, sites - 1):
            pl.semaphore_signal(ready.at[n], inc=1, device_id=to_site(d), device_id_type=MESH)

    def told(n):
        pl.semaphore_wait(ready.at[n], 2)

    def hop(j, i, block, lo, hi, device):
        ref = amps.at[j, block, pl.ds(lo, hi - lo)]
        return pltpu.make_async_remote_copy(
            src_ref=ref, dst_ref=ref, send_sem=sends.at[0], recv_sem=a_recv.at[j, GROUP[i]],
            device_id=device, device_id_type=MESH,
        )

    hops = (
        (row, down, 0, kets, to_up),
        (row, up, 0, kets, to_down),
        (row, over, 0, kets, to_over),
        (down, two, 0, HALF, to_up),
        (down, down_o, 0, FIRST, to_over),
        (up, two, HALF, kets, to_down),
        (up, up_o, 0, FIRST, to_over),
        (over, down_o, FIRST, kets, to_up),
        (over, up_o, FIRST, kets, to_down),
        (two, two_o, 0, FIRST, to_over),
        (down_o, two_o, FIRST, FIRST + QUARTER, to_up),
        (up_o, two_o, FIRST + QUARTER, kets, to_down),
    )

    def send(j, i):
        block, _, lo, hi, device = hops[i]
        hop(j, i, block, lo, hi, device).start()

    def landed(ref, sem):
        pltpu.make_async_copy(ref, ref, sem).wait()

    def arrived(j, group):
        count = sum(hi - lo for (_, _, lo, hi, _), g in zip(hops, GROUP) if g == group)
        parts_ = next(n for n in range(1, rows) if count % (n * 16) == 0 and count // n <= kets)
        landed(amps.at[j, pl.ds(0, parts_), pl.ds(0, count // parts_)], a_recv.at[j, group])

    def first(j):
        for i in (0, 1, 2):
            send(j, i)

    def second(j):
        arrived(j, 0)
        for i in (3, 7, 8, 5, 4, 6):
            send(j, i)

    def third(j):
        arrived(j, 1)
        for i in (10, 11, 9):
            send(j, i)

    def gathered(j):
        arrived(j, 2)
        arrived(j, 3)

    def site(d):
        return lax.rem(z + d, sites)

    last = chunks - 1

    def sib_sem(j, d):
        return j if j < last else last + min(d, sites - 1 - d)

    def sib_copy(j, d):
        return pltpu.make_async_remote_copy(
            src_ref=part.at[j, site(d), 1 - core], dst_ref=sib.at[j, site(d)],
            send_sem=sends.at[1], recv_sem=d_recv.at[sib_sem(j, d)],
            device_id=to_sib, device_id_type=MESH,
        )

    def multiply(j):
        for d in range(sites // 2, sites):
            both = (d, sites - 1 - d)
            left = jnp.concatenate([screened[pl.ds(site(e) * 128, 128), :] for e in both], axis=0)
            right = amps[j].reshape(rows * kets, width)
            product = jnp.dot(left, right, preferred_element_type=jnp.float32).reshape(2, 2, 64, width)
            for i, e in enumerate(both):
                part[j, site(e)] = product[i]
                sib_copy(j, e).start()

    def summed(j, d):
        return part[j, site(d), core] + sib[j, site(d)]

    def encode(j, slot, value):
        top = jnp.maximum(jnp.max(jnp.abs(value), axis=0, keepdims=True), 1e-30)
        scale[j, slot] = top * (1.0 / LEVELS)
        quant[j, slot] = jnp.round(value * (LEVELS / top)).astype(jnp.int32).astype(jnp.int16)

    def decode(code, factor):
        return code.astype(jnp.int32).astype(jnp.float32) * factor

    def message(j, slot, inbox, factor, lo, hi, d, group):
        device = to_site(d)
        return (
            pltpu.make_async_remote_copy(
                src_ref=scale.at[j, slot], dst_ref=zscale.at[j, factor],
                send_sem=sends.at[3], recv_sem=s_recv.at[j, group], device_id=device, device_id_type=MESH,
            ),
            pltpu.make_async_remote_copy(
                src_ref=quant.at[j, slot, pl.ds(lo, hi - lo)], dst_ref=zin.at[j, inbox, pl.ds(lo, hi - lo)],
                send_sem=sends.at[2], recv_sem=z_recv.at[j, group], device_id=device, device_id_type=MESH,
            ),
        )

    def post(*args):
        for c in message(*args):
            c.start()

    def await_sib(j):
        with jax.named_scope("sibwait"):
            landed(sib.at[j], d_recv.at[j])

    def scatter(j):
        await_sib(j)
        encode(j, 2, summed(j, 4))
        post(j, 2, 2, 2, 0, 32, 2, 0)
        post(j, 2, 2, 3, 32, 64, 6, 0)
        encode(j, 0, summed(j, 3))
        post(j, 0, 0, 0, 0, 64, 1, 0)
        encode(j, 1, summed(j, 5))
        post(j, 1, 1, 1, 0, 64, 7, 0)
        encode(j, 3, summed(j, 1))
        post(j, 3, 3, 4, 0, 64, 1, 1)
        encode(j, 4, summed(j, 7))
        post(j, 4, 4, 5, 0, 64, 7, 1)

    def relay(j):
        with jax.named_scope("relaywait"):
            landed(zscale.at[j, pl.ds(0, 4)], s_recv.at[j, 0])
            landed(zin.at[j, pl.ds(0, 3)], z_recv.at[j, 0])
        ahead = summed(j, 2) + decode(zin[j, 0], zscale[j, 0])
        top = decode(zin[j, 2, 0:32], zscale[j, 2])
        encode(j, 5, jnp.concatenate([ahead[0:32] + top, ahead[32:64]], axis=0))
        post(j, 5, 5, 6, 0, 64, 2, 1)
        behind = summed(j, 6) + decode(zin[j, 1], zscale[j, 1])
        low = decode(zin[j, 2, 32:64], zscale[j, 3])
        encode(j, 6, jnp.concatenate([behind[0:32], behind[32:64] + low], axis=0))
        post(j, 6, 6, 7, 0, 64, 6, 1)

    def pair_copy(j):
        return pltpu.make_async_remote_copy(
            src_ref=total.at[j, pl.ds((1 - pair) * 32, 32)], dst_ref=pair_in.at[j],
            send_sem=sends.at[4], recv_sem=p_recv.at[j],
            device_id=to_pair, device_id_type=MESH,
        )

    def collect(j):
        value = summed(j, 0)
        with jax.named_scope("sitewait"):
            landed(zscale.at[j, pl.ds(4, 4)], s_recv.at[j, 1])
            landed(zin.at[j, pl.ds(3, 4)], z_recv.at[j, 1])
        for i in range(4):
            value += decode(zin[j, 3 + i], zscale[j, 4 + i])
        total[j] = value
        pair_copy(j).start()

    near = chunks - FAR

    def far_copies(j, d, other):
        whom = 1 - pair if other else pair
        device = (row, site(d) * 2 + core, whom)
        f = j - near
        return (
            pltpu.make_async_remote_copy(
                src_ref=scale.at[j, d], dst_ref=far_scale.at[f, other, d],
                send_sem=sends.at[5 + other], recv_sem=f_recv.at[f, other], device_id=device, device_id_type=MESH,
            ),
            pltpu.make_async_remote_copy(
                src_ref=quant.at[j, d, pl.ds(whom * 32, 32)], dst_ref=far.at[f, other, d],
                send_sem=sends.at[7 + other], recv_sem=f_recv.at[f, 2 + other], device_id=device, device_id_type=MESH,
            ),
        )

    def scatter_far(j):
        if j < last:
            await_sib(j)
        for d in range(sites // 2, sites):
            if j == last:
                with jax.named_scope("sibwait"):
                    landed(sib.at[j, pl.ds(0, 2)], d_recv.at[sib_sem(j, d)])
            for e in (d, sites - 1 - d):
                encode(j, e, summed(j, e))
                for other in (1, 0) if e else (1,):
                    for c in far_copies(j, e, other):
                        c.start()

    def finish_far(j):
        f = j - near
        for other in (0, 1):
            first_ = 0 if other else 1
            with jax.named_scope("farwait"):
                landed(far_scale.at[f, other, pl.ds(first_, sites - first_)], f_recv.at[f, other])
                landed(far.at[f, other, pl.ds(first_, sites - first_)], f_recv.at[f, 2 + other])
            ladder = decode(far[f, other, first_], far_scale[f, other, first_])
            for d in range(first_ + 1, sites):
                ladder += decode(far[f, other, d], far_scale[f, other, d])
            if not other:
                ladder += part[j, z, core, pl.ds(pair * 32, 32)] + sib[j, z, pl.ds(pair * 32, 32)]
            couple(j, 1 - pair if other else pair, ladder)

    def far_sent():
        for other in (0, 1):
            first_ = 0 if other else 1
            landed(far_scale.at[:, other, pl.ds(first_, sites - first_)], sends.at[5 + other])
            landed(far.at[:, other, pl.ds(first_, sites - first_)], sends.at[7 + other])

    half = chunks * width

    def couple(j, which, ladder):
        columns = pl.ds(pl.multiple_of(which * half + j * width, width), width)
        residual = driver_v[:, columns].astype(jnp.float32) + ladder
        resid[:, columns] = residual
        scaled = (residual / (vir_col() - occ_v[columns].reshape(1, width))).astype(jnp.bfloat16)
        coupled[...] += jnp.dot(scaled, coup_v[columns, :], preferred_element_type=jnp.float32)

    def vir_col():
        n = vir_v.shape[0]
        eye = lax.broadcasted_iota(jnp.int32, (n, n), 0) == lax.broadcasted_iota(jnp.int32, (n, n), 1)
        return jnp.sum(jnp.where(eye, jnp.broadcast_to(vir_v[...].reshape(1, n), (n, n)), 0.0), axis=1, keepdims=True)

    def finish(j):
        couple(j, pair, total[j, pl.ds(pair * 32, 32)])
        with jax.named_scope("pairwait"):
            pair_copy(j).wait_recv()
        couple(j, 1 - pair, pair_in[j])

    with jax.named_scope("barrier"):
        pl.semaphore_wait(barrier, len(friends))
    landed(amps.at[:, row], load_sem.at[6])
    with jax.named_scope("first"):
        for j in range(min(AHEAD, chunks)):
            first(j)
    tell(0)

    coupled[...] = jnp.zeros_like(coupled)
    loads[0].wait()
    tiles = kept_v.shape[1]
    tile = depth // tiles
    keep = kept_v[...].astype(jnp.float32).astype(jnp.bfloat16)
    for b in range(depth // 256):
        ket = lax.broadcasted_iota(jnp.int32, (tiles, 256), 1) + b * 256
        of = lax.broadcasted_iota(jnp.int32, (tiles, 256), 0) * tile
        spread = jnp.where((ket >= of) & (ket < of + tile), 1.0, 0.0).astype(jnp.bfloat16)
        mask[:, pl.ds(b * 256, 256)] = jnp.dot(keep, spread, preferred_element_type=jnp.float32)
    loads[1].wait()

    def screen(i, carry):
        strip = pl.ds(i * tile, tile)
        keep_row = jnp.broadcast_to(mask[pl.ds(i, 1), :], (tile, depth)).astype(jnp.bfloat16)
        screened[strip, :] = screened[strip, :] * keep_row
        return carry

    with jax.named_scope("screen"):
        lax.fori_loop(0, kept_v.shape[0], screen, 0)
    def product(j):
        with jax.named_scope("gathered"):
            gathered(j)
        with jax.named_scope("dot"):
            multiply(j)

    def named(name, f):
        def call(j):
            with jax.named_scope(name):
                f(j)

        return call

    steps = {
        "S": (0, named("second", second)),
        "F": (-AHEAD, first),
        "T": (LAG_T, named("third", third)),
        "G": (LAG_G, product),
        "X": (LAG_G + 1, lambda j: scatter(j) if j < near else scatter_far(j)),
        "R": (LAG_G + 2, relay),
        "C": (LAG_G + 4, collect),
        "E": (LAG_G + 20, finish),
    }
    done = dict.fromkeys(steps, -1)
    done["F"] = AHEAD - 1
    for s in range(chunks + LAG_G):
        for name in ORDER:
            lag, step = steps[name]
            j = s - lag
            if 0 <= j < (near if name in "RCE" else chunks) and j > done[name]:
                step(j)
                done[name] = j
        if s < sites // 2 - 1:
            told(s)
            if s + 1 < sites // 2 - 1:
                tell(s + 1)
        if s == 2:
            pl.semaphore_signal(ready.at[sites // 2 - 1], inc=1, device_id=to_pair, device_id_type=MESH)
            for c in loads[2:]:
                c.wait()
    pl.semaphore_wait(ready.at[sites // 2 - 1], 1)
    for j in range(done["X"] + 1, chunks):
        steps["X"][1](j)
    for j in range(done["R"] + 1, near):
        relay(j)
    for j in range(done["C"] + 1, near):
        while done["E"] < j - 2:
            done["E"] += 1
            finish(done["E"])
        collect(j)
    landed(amps.at[:, pl.ds(0, rows - 1)], sends.at[0])
    landed(sib, sends.at[1])
    landed(zin, sends.at[2])
    landed(zscale, sends.at[3])
    for j in range(done["E"] + 1, near - 1):
        finish(j)
    for j in range(near, last):
        finish_far(j)
    finish(near - 1)
    far_sent()
    landed(pair_in.at[pl.ds(0, near)], sends.at[4])
    finish_far(last)
    with jax.named_scope("out"):
        resid[...] = resid[...] - coupled[...]
        oc = pltpu.make_async_copy(resid, out, load_sem.at[6])
        oc.start()
        oc.wait()


def per_device(integrals, kept_tiles, amplitudes, driver, vir_energy, occ_energy, occ_coupling):
    bra, depth = integrals.shape
    kets, half = amplitudes.shape
    rows = depth // kets
    chunks = half // WIDTH
    sites = bra // 128
    own, whole = driver.shape
    any_ = pl.BlockSpec(memory_space=pltpu.HBM)
    dma = pltpu.SemaphoreType.DMA
    numerator = pl.pallas_call(
        kernel,
        out_shape=jax.ShapeDtypeStruct((own, whole), jnp.float32),
        in_specs=[any_] * 7,
        out_specs=any_,
        scratch_shapes=[
            pltpu.VMEM((bra, depth), jnp.bfloat16),
            pltpu.VMEM(kept_tiles.shape, jnp.int32),
            pltpu.VMEM((own, whole), jnp.bfloat16),
            pltpu.VMEM((own,), jnp.float32),
            pltpu.VMEM((whole,), jnp.float32),
            pltpu.VMEM((whole, whole), jnp.bfloat16),
            pltpu.VMEM((kept_tiles.shape[0], depth), jnp.float32),
            pltpu.VMEM((chunks, rows, kets, WIDTH), jnp.bfloat16),
            pltpu.VMEM((chunks, sites, 2, 64, WIDTH), jnp.float32),
            pltpu.VMEM((chunks, sites, 64, WIDTH), jnp.float32),
            pltpu.VMEM((chunks, sites, 64, WIDTH), jnp.int16),
            pltpu.VMEM((chunks, sites, 1, WIDTH), jnp.float32),
            pltpu.VMEM((chunks - FAR, 7, 64, WIDTH), jnp.int16),
            pltpu.VMEM((chunks - FAR, 8, 1, WIDTH), jnp.float32),
            pltpu.VMEM((chunks, 64, WIDTH), jnp.float32),
            pltpu.VMEM((chunks, 32, WIDTH), jnp.float32),
            pltpu.VMEM((FAR, 2, sites, 32, WIDTH), jnp.int16),
            pltpu.VMEM((FAR, 2, sites, 1, WIDTH), jnp.float32),
            pltpu.VMEM((own, whole), jnp.float32),
            pltpu.VMEM((own, whole), jnp.float32),
            dma((7,)),
            dma((9,)),
            dma((chunks, 4)),
            dma((chunks + sites // 2,)),
            dma((chunks, 2)),
            dma((chunks, 2)),
            dma((chunks,)),
            dma((FAR, 4)),
            pltpu.SemaphoreType.REGULAR((sites // 2,)),
        ],
        compiler_params=pltpu.CompilerParams(
            collective_id=0, has_side_effects=True, vmem_limit_bytes=60 * 1024 * 1024
        ),
        name="ladder",
    )(
        integrals, kept_tiles, amplitudes, driver,
        vir_energy, occ_energy, occ_coupling,
    )
    return -numerator / (vir_energy[:, None] - occ_energy[None, :])


def solution(mesh):
    place = ("row", "col", "pair")
    placed = (
        P("row", "col"),
        P("row", "col"),
        P(("col", "row"), "pair"),
        P(place, None),
        P(place),
        P(),
        P(),
    )
    return jax.shard_map(
        per_device, mesh=mesh, in_specs=placed, out_specs=P(place, None), check_vma=False
    )
```
